32 devices in a mesh: groups: 2 (over x), replica: 16 (over z, y, core).
Axes of the slice: x: 2, y: 2, z: 4, core: 2. Of those that a mesh axis runs over, the one named last changes fastest.
Arguments:
- tokens: bfloat16 [32768, 2048], P(('groups', 'replica')), parts along dimension 0, may hold values from -6 to 6
- pseudo_keys: bfloat16 [32, 2048, 512], P(('groups', 'replica')), parts along dimension 0, may hold values from -0.875 to 0.875
- pseudo_values: bfloat16 [32, 2048, 512], P(('groups', 'replica')), parts along dimension 0, may hold values from -0.875 to 0.875
- master_keys: float32 [4096, 512], P(('groups', 'replica')), parts along dimension 0, may hold values from -0.125 to 0.125
- moment_keys: float32 [4096, 512], P(('groups', 'replica')), parts along dimension 0, may hold values from -0.125 to 0.125
- master_values: float32 [4096, 512], P(('groups', 'replica')), parts along dimension 0, may hold values from -0.125 to 0.125
- moment_values: float32 [4096, 512], P(('groups', 'replica')), parts along dimension 0, may hold values from -0.125 to 0.125
- outer_hyper: float32 [4], P('groups'), parts along dimension 0, may hold values from 0.5 to 0.95
Outputs:
- eval_keys: bfloat16 [32768, 512], P(('groups', 'replica')), parts along dimension 0
- eval_values: bfloat16 [32768, 512], P(('groups', 'replica')), parts along dimension 0
- new_master_keys: float32 [4096, 512], P(('groups', 'replica')), parts along dimension 0
- new_moment_keys: float32 [4096, 512], P(('groups', 'replica')), parts along dimension 0
- new_master_values: float32 [4096, 512], P(('groups', 'replica')), parts along dimension 0
- new_moment_values: float32 [4096, 512], P(('groups', 'replica')), parts along dimension 0
The draws below stay inside these ranges and needn't reach their ends.
There are 2 independent parts, one for each index of `groups`. The reference program is written for one: setup_inputs(seed, part) draws one part's arguments, and reference() takes and returns one part's arrays. A program takes and returns all parts, laid end to end along the dimension named above; each array names one. Nothing has to cross between parts.
All inputs are finite; a program needn't handle non-finite values.
Results may differ from the reference program's by a relative error of at most 0.0049.
Values may be sent and summed in bfloat16 or wider, within the bound.
A program may use at most 128 MiB of HBM per device.

```python
import jax
import jax.numpy as jnp

D = 2048
KVW = 512
TOKENS = 16384
N_REPLICA = 16


def with_spikes(array, stream_key, source, target, blocks, factor):
    owner, partner = [(jnp.arange(array.shape[position]) // (array.shape[position] // blocks)).reshape([-1 if axis == position else 1 for axis in range(array.ndim)]) for position in (source, target)]
    chosen = jax.random.permutation(stream_key, blocks)[partner]
    strong = (owner == chosen) | (owner == (partner + blocks // 2) % blocks)
    return jnp.where(strong, factor * array, array)


def levels(rng, shape, pieces, least, high):
    def one(dim, shards_of):
        heights = jax.random.uniform(jax.random.fold_in(jax.random.fold_in(rng, 6), dim), (shards_of,), jnp.float32, least / len(pieces), high / len(pieces))
        return jnp.repeat(jnp.exp(heights), shape[dim] // shards_of).reshape((-1,) + (1,) * (len(shape) - dim - 1))

    loudness = one(*pieces[0])
    for cut in pieces[1:]:
        loudness = loudness * one(*cut)
    return loudness


def gaussian(rng, dims, spread, limit, pieces=(), held_as=jnp.bfloat16):
    values = spread * jax.random.normal(rng, dims, jnp.float32)
    if pieces:
        values = values * levels(rng, dims, pieces, -0.22, 0.18)
    return jnp.clip(values, -limit, limit).astype(held_as)


def bell_draw_with(stream_key, dims, deviation, limit, pieces, heavy, dtype=jnp.bfloat16):
    drawn = deviation * jax.random.normal(stream_key, dims, jnp.float32)
    if pieces:
        drawn = drawn * levels(stream_key, dims, pieces, -0.22, 0.18)
    return jnp.clip(with_spikes(drawn, jax.random.fold_in(stream_key, 3), *heavy), -limit, limit).astype(dtype)


def setup_inputs(seed: int = 0, part: int = 0) -> dict:
    arg_keys = jax.random.split(jax.random.key(seed), 9)
    part_keys = jax.random.split(jax.random.fold_in(arg_keys[8], part), 9)
    return {
        "tokens": gaussian(part_keys[0], (TOKENS, D), 1.0, 6.0, ((0, 16),)),
        "pseudo_keys": bell_draw_with(part_keys[1], (N_REPLICA, D, KVW), 0.1, 0.875, ((0, 16),), (0, 1, 16, 2.0)),
        "pseudo_values": bell_draw_with(part_keys[2], (N_REPLICA, D, KVW), 0.1, 0.875, ((0, 16),), (0, 1, 16, 2.0)),
        "master_keys": gaussian(part_keys[3], (D, KVW), D ** -0.5, 0.125, ((0, 16),), jnp.float32),
        "moment_keys": gaussian(part_keys[4], (D, KVW), 0.02, 0.125, ((0, 16),), jnp.float32),
        "master_values": gaussian(part_keys[5], (D, KVW), D ** -0.5, 0.125, ((0, 16),), jnp.float32),
        "moment_values": gaussian(part_keys[6], (D, KVW), 0.02, 0.125, ((0, 16),), jnp.float32),
        "outer_hyper": jnp.clip(jax.random.uniform(part_keys[7], (2,), jnp.float32, 0.5, 0.95), 0.5, 0.95),
    }


def outer_update(pseudo, master, moment, outer_rate, outer_mom):
    averaged = jnp.sum(pseudo.astype(jnp.float32), axis=0) / N_REPLICA
    moment_new = outer_mom * moment + averaged
    master_new = master - outer_rate * (averaged + outer_mom * moment_new)
    return master_new, moment_new


def reference(tokens, pseudo_keys, pseudo_values, master_keys, moment_keys, master_values, moment_values, outer_hyper):
    outer_rate = outer_hyper[0]
    outer_mom = outer_hyper[1]
    master_k, moment_k = outer_update(pseudo_keys, master_keys, moment_keys, outer_rate, outer_mom)
    master_v, moment_v = outer_update(pseudo_values, master_values, moment_values, outer_rate, outer_mom)
    eval_keys = jnp.dot(tokens, master_k.astype(jnp.bfloat16), preferred_element_type=jnp.float32).astype(jnp.bfloat16)
    eval_values = jnp.dot(tokens, master_v.astype(jnp.bfloat16), preferred_element_type=jnp.float32).astype(jnp.bfloat16)
    return (eval_keys, eval_values, master_k, moment_k, master_v, moment_v)
```

```python
import functools

import jax
import jax.numpy as jnp
from jax import lax
from jax.experimental import pallas as pl
from jax.experimental.pallas import tpu as pltpu
from jax.sharding import PartitionSpec as P

MESH = pl.DeviceIdType.MESH
F32 = jnp.float32
BF16 = jnp.bfloat16


def kernel(
    Z,
    Y,
    replicas,
    tokens,
    pseudo_keys,
    pseudo_values,
    master_keys,
    moment_keys,
    master_values,
    moment_values,
    hyper,
    eval_keys,
    eval_values,
    out_master_keys,
    out_moment_keys,
    out_master_values,
    out_moment_values,
    tok,
    mine,
    from_core,
    to_y,
    from_y,
    to_z,
    from_left,
    from_right,
    weights,
    total,
    acc,
    result,
    master,
    moment,
    load_sem,
    state_sem,
    tok_sem,
    store_sem,
    rc_s,
    rc_r,
    ry_s,
    ry_r,
    rz_s,
    rl_r,
    rr_r,
    gr_s,
    gl_s,
    gz_r,
    gy_s,
    gy_r,
    gc_s,
    gc_r,
):
    me = lax.axis_index("replica")
    core = lax.rem(me, 2)
    chip = lax.div(me, 2)
    y = lax.rem(chip, Y)
    z = lax.div(chip, Y)
    oc = 1 - core
    oy = 1 - y

    def dev(zz, yy, cc):
        return {"replica": (zz * Y + yy) * 2 + cc}

    pseudo = (pseudo_keys, pseudo_values)
    rows = mine.shape[3]

    loads = [
        pltpu.make_async_copy(pseudo[kv].at[:, :, core], mine.at[kv], load_sem.at[kv])
        for kv in range(2)
    ]
    states = [
        pltpu.make_async_copy(src, dst, state_sem.at[i])
        for i, (src, dst) in enumerate(
            (
                (master_keys, master.at[0]),
                (moment_keys, moment.at[0]),
                (master_values, master.at[1]),
                (moment_values, moment.at[1]),
            )
        )
    ]
    blocks = tok.shape[0]
    depth = tok.shape[2]
    if len(tokens.shape) == 3:
        tok_loads = [
            pltpu.make_async_copy(tokens.at[q], tok.at[q], tok_sem.at[q]) for q in range(blocks)
        ]
    else:
        tok_loads = [
            pltpu.make_async_copy(
                tokens.at[:, q * depth : (q + 1) * depth], tok.at[q], tok_sem.at[q]
            )
            for q in range(blocks)
        ]

    def near(s):
        m = jnp.minimum(z, Z - 1 - z)
        half = lax.div(s + 1, 2)
        side = 2 * lax.rem(s + 1, 2) - 1
        beyond = jnp.where(z < Z - 1 - z, s, Z - 1 - s)
        return jnp.where(s <= 2 * m, z + half * side, beyond)

    def far(s):
        return near(Z - 1 - s)

    def steps(count, body, start=0):
        def run(s, carry):
            body(s)
            return carry

        lax.fori_loop(start, count, run, 0)

    def remote(src, dst, send, recv, device):
        return pltpu.make_async_remote_copy(
            src_ref=src,
            dst_ref=dst,
            send_sem=send,
            recv_sem=recv,
            device_id=device,
            device_id_type=MESH,
        )

    def core_copy(kv, p):
        return remote(
            pseudo[kv].at[p, :, oc],
            from_core.at[kv, p],
            rc_s.at[kv, p],
            rc_r.at[kv, p],
            dev(z, y, oc),
        )

    def y_copy(kv, p):
        return remote(
            to_y.at[kv, p], from_y.at[kv, p], ry_s.at[kv, p], ry_r.at[kv, p], dev(z, oy, core)
        )

    def right_copy(kv, p):
        return remote(
            to_z.at[kv, p], from_left.at[kv, p], rz_s.at[kv, p], rl_r.at[kv, p], dev(z + 1, y, core)
        )

    def left_copy(kv, p):
        return remote(
            to_z.at[kv, p], from_right.at[kv, p], rz_s.at[kv, p], rr_r.at[kv, p], dev(z - 1, y, core)
        )

    def w_right(kv, p):
        w = weights.at[kv, p, y, core]
        return remote(w, w, gr_s.at[kv, p], gz_r.at[kv, p], dev(z + 1, y, core))

    def w_left(kv, p):
        w = weights.at[kv, p, y, core]
        return remote(w, w, gl_s.at[kv, p], gz_r.at[kv, p], dev(z - 1, y, core))

    def w_y(kv, p, yy):
        w = weights.at[kv, p, yy, core]
        return remote(w, w, gy_s.at[kv, p], gy_r.at[kv, p], dev(z, oy, core))

    def w_core(kv, p, yy, cc):
        w = weights.at[kv, p, yy, cc]
        return remote(w, w, gc_s.at[kv, p, yy], gc_r.at[kv, p, yy], dev(z, y, oc))

    for copy in loads:
        copy.start()

    barrier = pltpu.get_barrier_semaphore()
    pl.semaphore_signal(barrier, inc=1, device_id=dev(z, y, oc), device_id_type=MESH)
    pl.semaphore_signal(barrier, inc=1, device_id=dev(z, oy, core), device_id_type=MESH)

    @pl.when(z > 0)
    def _():
        pl.semaphore_signal(barrier, inc=1, device_id=dev(z - 1, y, core), device_id_type=MESH)

    @pl.when(z < Z - 1)
    def _():
        pl.semaphore_signal(barrier, inc=1, device_id=dev(z + 1, y, core), device_id_type=MESH)

    peers = 2 + jnp.where(z > 0, 1, 0) + jnp.where(z < Z - 1, 1, 0)
    pl.semaphore_wait(barrier, peers)

    for kv in range(2):
        steps(Z, lambda s: core_copy(kv, far(s)).start())
    for copy in states + tok_loads:
        copy.start()

    for kv in range(2):
        loads[kv].wait()

        def y_send(s):
            p = far(s)
            core_copy(kv, p).wait_recv()
            both = mine[kv, p, oy].astype(F32) + from_core[kv, p, oy].astype(F32)
            to_y[kv, p] = both.astype(BF16)
            y_copy(kv, p).start()

        steps(Z, y_send)

    acc[...] = jnp.zeros_like(acc)

    def reduce_step(kv, s):
        p = far(s)
        y_copy(kv, p).wait_recv()
        total[...] = (
            mine[kv, p, y].astype(F32)
            + from_core[kv, p, y].astype(F32)
            + from_y[kv, p].astype(F32)
        )

        @pl.when((p >= z) & (z > 0))
        def _():
            right_copy(kv, p).wait_recv()
            total[...] += from_left[kv, p].astype(F32)

        @pl.when((p <= z) & (z < Z - 1))
        def _():
            left_copy(kv, p).wait_recv()
            total[...] += from_right[kv, p].astype(F32)

        @pl.when(p != z)
        def _():
            to_z[kv, p] = total[...].astype(BF16)

        @pl.when(p > z)
        def _():
            right_copy(kv, p).start()

        @pl.when(p < z)
        def _():
            left_copy(kv, p).start()

    def nesterov(kv):
        outer_rate = hyper[0]
        outer_mom = hyper[1]
        averaged = total[...] / replicas
        moment_new = outer_mom * moment[kv] + averaged
        master_new = master[kv] - outer_rate * (averaged + outer_mom * moment_new)
        weights[kv, z, y, core] = master_new.astype(BF16)
        master[kv] = master_new
        moment[kv] = moment_new

    def spread(kv, p):
        @pl.when((p <= z) & (z < Z - 1))
        def _():
            w_right(kv, p).start()

        @pl.when((p >= z) & (z > 0))
        def _():
            w_left(kv, p).start()

        w_y(kv, p, y).start()
        w_core(kv, p, y, core).start()

    def gather_step(kv, s):
        p = near(s)
        w_right(kv, p).wait_recv()
        spread(kv, p)

    def dot(kv, p, yy):
        w_core(kv, p, yy, oc).wait_recv()
        q = p * Y + yy
        block = weights[kv, p, yy].reshape(2 * rows, -1)
        tile = min(256, acc.shape[1])

        def one(m, carry):
            span = pl.ds(pl.multiple_of(m * tile, tile), tile)
            acc[kv, span, :] += jnp.dot(tok[q, span, :], block, preferred_element_type=F32)
            return carry

        lax.fori_loop(0, acc.shape[1] // tile, one, 0)

    def y_arrival(kv, s):
        p = near(s)
        w_y(kv, p, oy).wait_recv()
        w_core(kv, p, oy, core).start()

    outs = ((out_master_keys, out_moment_keys), (out_master_values, out_moment_values))

    def stores(kv):
        return [
            pltpu.make_async_copy(master.at[kv], outs[kv][0], store_sem.at[2 * kv]),
            pltpu.make_async_copy(moment.at[kv], outs[kv][1], store_sem.at[2 * kv + 1]),
        ]

    evals = [
        pltpu.make_async_copy(result.at[kv], out, store_sem.at[4 + kv])
        for kv, out in enumerate((eval_keys, eval_values))
    ]

    steps(Z, lambda s: reduce_step(0, s))
    states[0].wait()
    states[1].wait()
    nesterov(0)
    spread(0, z)
    for copy in stores(0):
        copy.start()

    def reduce_and_gather(s):
        reduce_step(1, s)
        gather_step(0, s + 1)

    steps(Z - 1, reduce_and_gather)
    reduce_step(1, Z - 1)
    states[2].wait()
    states[3].wait()
    nesterov(1)
    spread(1, z)
    for copy in stores(1):
        copy.start()
    for copy in tok_loads:
        copy.wait()

    def second(s):
        dot(0, near(s), y)
        gather_step(1, s + 1)
        y_arrival(0, s)

    steps(Z - 1, second)
    y_arrival(0, Z - 1)
    dot(0, near(Z - 1), y)
    steps(Z, lambda s: dot(0, near(s), oy))
    result[0] = acc[0].astype(BF16)
    evals[0].start()
    steps(Z, lambda s: dot(1, near(s), y))

    def last(s):
        y_arrival(1, s)
        dot(1, near(s), oy)

    steps(Z, last)
    result[1] = acc[1].astype(BF16)
    evals[1].start()

    for kv in range(2):

        def drain(p):
            core_copy(kv, p).wait_send()
            y_copy(kv, p).wait_send()

            @pl.when(p != z)
            def _():
                right_copy(kv, p).wait_send()

            @pl.when((p <= z) & (z < Z - 1))
            def _():
                w_right(kv, p).wait_send()

            @pl.when((p >= z) & (z > 0))
            def _():
                w_left(kv, p).wait_send()

            w_y(kv, p, y).wait_send()
            w_core(kv, p, y, core).wait_send()
            w_core(kv, p, oy, core).wait_send()

        steps(Z, drain)
        for copy in stores(kv):
            copy.wait()
    for copy in evals:
        copy.wait()


def body(
    tokens,
    pseudo_keys,
    pseudo_values,
    master_keys,
    moment_keys,
    master_values,
    moment_values,
    outer_hyper,
):
    replicas = lax.axis_size("replica")
    Y = 2
    Z = replicas // (2 * Y)
    width = master_keys.shape[1]
    rows = master_keys.shape[0]
    count = tokens.shape[0]
    blocks = Z * Y
    depth = 2 * rows
    if depth % 128:
        tokens = tokens.reshape(count, blocks, depth).swapaxes(0, 1)
    pseudo_keys, pseudo_values = (
        p.reshape(Z, Y, 2, rows, width) for p in (pseudo_keys, pseudo_values)
    )
    hbm = pl.BlockSpec(memory_space=pl.ANY)
    dma = pltpu.SemaphoreType.DMA
    state = jax.ShapeDtypeStruct(master_keys.shape, F32)
    evaluated = jax.ShapeDtypeStruct((count, width), BF16)
    part = pltpu.VMEM((2, Z, rows, width), BF16)
    pair = pltpu.VMEM((2, Z, Y, rows, width), BF16)
    unit = dma((2, Z))
    return pl.pallas_call(
        functools.partial(kernel, Z, Y, replicas),
        out_shape=(evaluated, evaluated, state, state, state, state),
        in_specs=[hbm] * 7 + [pl.BlockSpec(memory_space=pltpu.SMEM)],
        out_specs=(hbm,) * 6,
        scratch_shapes=[
            pltpu.VMEM((blocks, count, depth), BF16),
            pair,
            pair,
            part,
            part,
            part,
            part,
            part,
            pltpu.VMEM((2, Z, Y, 2, rows, width), BF16),
            pltpu.VMEM((rows, width), F32),
            pltpu.VMEM((2, count, width), F32),
            pltpu.VMEM((2, count, width), BF16),
            pltpu.VMEM((2, rows, width), F32),
            pltpu.VMEM((2, rows, width), F32),
            dma((2,)),
            dma((4,)),
            dma((blocks,)),
            dma((6,)),
            unit,
            unit,
            unit,
            unit,
            unit,
            unit,
            unit,
            unit,
            unit,
            unit,
            unit,
            unit,
            dma((2, Z, Y)),
            dma((2, Z, Y)),
        ],
        compiler_params=pltpu.CompilerParams(
            collective_id=0, has_side_effects=True, vmem_limit_bytes=60 * 1024 * 1024
        ),
        name="outer_step",
    )(
        tokens,
        pseudo_keys,
        pseudo_values,
        master_keys,
        moment_keys,
        master_values,
        moment_values,
        outer_hyper,
    )


def solution(mesh):
    rows = P(("groups", "replica"), None)
    stack = P(("groups", "replica"), None, None)
    return jax.shard_map(
        body,
        mesh=mesh,
        in_specs=(rows, stack, stack, rows, rows, rows, rows, P("groups")),
        out_specs=(rows,) * 6,
        check_vma=False,
    )
```

```python
import functools

import jax
import jax.numpy as jnp
from jax import lax
from jax.experimental import pallas as pl
from jax.experimental.pallas import tpu as pltpu
from jax.sharding import PartitionSpec as P

MESH = pl.DeviceIdType.MESH
F32 = jnp.float32
BF16 = jnp.bfloat16


def kernel(
    Z,
    Y,
    replicas,
    tokens,
    pseudo_keys,
    pseudo_values,
    master_keys,
    moment_keys,
    master_values,
    moment_values,
    hyper,
    eval_keys,
    eval_values,
    out_master_keys,
    out_moment_keys,
    out_master_values,
    out_moment_values,
    tok,
    mine,
    from_core,
    to_y,
    from_y,
    to_z,
    from_left,
    from_right,
    weights,
    total,
    acc,
    result,
    master,
    moment,
    load_sem,
    state_sem,
    tok_sem,
    store_sem,
    rc_s,
    rc_r,
    ry_s,
    ry_r,
    rz_s,
    rl_r,
    rr_r,
    gr_s,
    gl_s,
    gz_r,
    gy_s,
    gy_r,
    gc_s,
    gc_r,
):
    me = lax.axis_index("replica")
    core = lax.rem(me, 2)
    chip = lax.div(me, 2)
    y = lax.rem(chip, Y)
    z = lax.div(chip, Y)
    oc = 1 - core
    oy = 1 - y

    def dev(zz, yy, cc):
        return {"replica": (zz * Y + yy) * 2 + cc}

    pseudo = (pseudo_keys, pseudo_values)
    rows = mine.shape[3]

    loads = [
        pltpu.make_async_copy(pseudo[kv].at[:, :, core], mine.at[kv], load_sem.at[kv])
        for kv in range(2)
    ]
    states = [
        pltpu.make_async_copy(src, dst, state_sem.at[i])
        for i, (src, dst) in enumerate(
            (
                (master_keys, master.at[0]),
                (moment_keys, moment.at[0]),
                (master_values, master.at[1]),
                (moment_values, moment.at[1]),
            )
        )
    ]
    blocks = tok.shape[0]
    depth = tok.shape[2]
    if len(tokens.shape) == 3:
        tok_loads = [
            pltpu.make_async_copy(tokens.at[q], tok.at[q], tok_sem.at[q]) for q in range(blocks)
        ]
    else:
        tok_loads = [
            pltpu.make_async_copy(
                tokens.at[:, q * depth : (q + 1) * depth], tok.at[q], tok_sem.at[q]
            )
            for q in range(blocks)
        ]

    def near(s):
        m = jnp.minimum(z, Z - 1 - z)
        half = lax.div(s + 1, 2)
        side = 2 * lax.rem(s + 1, 2) - 1
        beyond = jnp.where(z < Z - 1 - z, s, Z - 1 - s)
        return jnp.where(s <= 2 * m, z + half * side, beyond)

    def far(s):
        return near(Z - 1 - s)

    def steps(count, body, start=0):
        def run(s, carry):
            body(s)
            return carry

        lax.fori_loop(start, count, run, 0)

    def remote(src, dst, send, recv, device):
        return pltpu.make_async_remote_copy(
            src_ref=src,
            dst_ref=dst,
            send_sem=send,
            recv_sem=recv,
            device_id=device,
            device_id_type=MESH,
        )

    def core_copy(kv, p):
        return remote(
            pseudo[kv].at[p, :, oc],
            from_core.at[kv, p],
            rc_s.at[kv, p],
            rc_r.at[kv, p],
            dev(z, y, oc),
        )

    def y_copy(kv, p):
        return remote(
            to_y.at[kv, p], from_y.at[kv, p], ry_s.at[kv, p], ry_r.at[kv, p], dev(z, oy, core)
        )

    def right_copy(kv, p):
        return remote(
            to_z.at[kv, p], from_left.at[kv, p], rz_s.at[kv, p], rl_r.at[kv, p], dev(z + 1, y, core)
        )

    def left_copy(kv, p):
        return remote(
            to_z.at[kv, p], from_right.at[kv, p], rz_s.at[kv, p], rr_r.at[kv, p], dev(z - 1, y, core)
        )

    def w_right(kv, p):
        w = weights.at[kv, p, y, core]
        return remote(w, w, gr_s.at[kv, p], gz_r.at[kv, p], dev(z + 1, y, core))

    def w_left(kv, p):
        w = weights.at[kv, p, y, core]
        return remote(w, w, gl_s.at[kv, p], gz_r.at[kv, p], dev(z - 1, y, core))

    def w_y(kv, p, yy):
        w = weights.at[kv, p, yy, core]
        return remote(w, w, gy_s.at[kv, p], gy_r.at[kv, p], dev(z, oy, core))

    def w_core(kv, p, yy, cc):
        w = weights.at[kv, p, yy, cc]
        return remote(w, w, gc_s.at[kv, p, yy], gc_r.at[kv, p, yy], dev(z, y, oc))

    for copy in loads:
        copy.start()

    barrier = pltpu.get_barrier_semaphore()
    pl.semaphore_signal(barrier, inc=1, device_id=dev(z, y, oc), device_id_type=MESH)
    pl.semaphore_signal(barrier, inc=1, device_id=dev(z, oy, core), device_id_type=MESH)

    @pl.when(z > 0)
    def _():
        pl.semaphore_signal(barrier, inc=1, device_id=dev(z - 1, y, core), device_id_type=MESH)

    @pl.when(z < Z - 1)
    def _():
        pl.semaphore_signal(barrier, inc=1, device_id=dev(z + 1, y, core), device_id_type=MESH)

    peers = 2 + jnp.where(z > 0, 1, 0) + jnp.where(z < Z - 1, 1, 0)
    pl.semaphore_wait(barrier, peers)

    for kv in range(2):
        steps(Z, lambda s: core_copy(kv, far(s)).start())
    for copy in states + tok_loads:
        copy.start()

    for kv in range(2):
        loads[kv].wait()

        def y_send(s):
            p = far(s)
            core_copy(kv, p).wait_recv()
            both = mine[kv, p, oy].astype(F32) + from_core[kv, p, oy].astype(F32)
            to_y[kv, p] = both.astype(BF16)
            y_copy(kv, p).start()

        steps(Z, y_send)

    acc[...] = jnp.zeros_like(acc)

    def reduce_step(kv, s):
        p = far(s)
        y_copy(kv, p).wait_recv()
        total[...] = (
            mine[kv, p, y].astype(F32)
            + from_core[kv, p, y].astype(F32)
            + from_y[kv, p].astype(F32)
        )

        @pl.when((p >= z) & (z > 0))
        def _():
            right_copy(kv, p).wait_recv()
            total[...] += from_left[kv, p].astype(F32)

        @pl.when((p <= z) & (z < Z - 1))
        def _():
            left_copy(kv, p).wait_recv()
            total[...] += from_right[kv, p].astype(F32)

        @pl.when(p != z)
        def _():
            to_z[kv, p] = total[...].astype(BF16)

        @pl.when(p > z)
        def _():
            right_copy(kv, p).start()

        @pl.when(p < z)
        def _():
            left_copy(kv, p).start()

    def nesterov(kv):
        outer_rate = hyper[0]
        outer_mom = hyper[1]
        averaged = total[...] / replicas
        moment_new = outer_mom * moment[kv] + averaged
        master_new = master[kv] - outer_rate * (averaged + outer_mom * moment_new)
        weights[kv, z, y, core] = master_new.astype(BF16)
        master[kv] = master_new
        moment[kv] = moment_new

    def spread(kv, p):
        @pl.when((p <= z) & (z < Z - 1))
        def _():
            w_right(kv, p).start()

        @pl.when((p >= z) & (z > 0))
        def _():
            w_left(kv, p).start()

        w_y(kv, p, y).start()
        w_core(kv, p, y, core).start()

    def gather_step(kv, s):
        p = near(s)
        w_right(kv, p).wait_recv()
        spread(kv, p)

    tile = min(1024, acc.shape[1])
    cols = 256
    across = acc.shape[2] // cols

    def dot(kv, p):
        for yy in range(Y):
            w_core(kv, p, yy, oc).wait_recv()

        def one(i, carry):
            m, n = lax.div(i, across), lax.rem(i, across)
            span = pl.ds(pl.multiple_of(m * tile, tile), tile)
            lane = pl.ds(pl.multiple_of(n * cols, cols), cols)
            part = acc[kv, span, lane]
            for yy in range(Y):
                block = weights[kv, p, yy, :, :, lane].reshape(2 * rows, cols)
                part += jnp.dot(tok[p * Y + yy, span, :], block, preferred_element_type=F32)
            acc[kv, span, lane] = part
            return carry

        lax.fori_loop(0, acc.shape[1] // tile * across, one, 0)

    def y_arrival(kv, s):
        p = near(s)
        w_y(kv, p, oy).wait_recv()
        w_core(kv, p, oy, core).start()

    outs = ((out_master_keys, out_moment_keys), (out_master_values, out_moment_values))

    def stores(kv):
        return [
            pltpu.make_async_copy(master.at[kv], outs[kv][0], store_sem.at[2 * kv]),
            pltpu.make_async_copy(moment.at[kv], outs[kv][1], store_sem.at[2 * kv + 1]),
        ]

    evals = [
        pltpu.make_async_copy(result.at[kv], out, store_sem.at[4 + kv])
        for kv, out in enumerate((eval_keys, eval_values))
    ]

    steps(Z, lambda s: reduce_step(0, s))
    states[0].wait()
    states[1].wait()
    nesterov(0)
    spread(0, z)
    for copy in stores(0):
        copy.start()

    reduce_step(1, 0)

    def reduce_and_gather(s):
        reduce_step(1, s)
        gather_step(0, s)

    steps(Z - 1, reduce_and_gather, 1)
    reduce_step(1, Z - 1)
    states[2].wait()
    states[3].wait()
    nesterov(1)
    spread(1, z)
    for copy in stores(1):
        copy.start()
    gather_step(0, Z - 1)
    for copy in tok_loads:
        copy.wait()

    def second(s):
        gather_step(1, s + 1)
        y_arrival(0, s)

    steps(Z - 1, second)
    y_arrival(0, Z - 1)
    steps(Z, lambda s: dot(0, near(s)))
    result[0] = acc[0].astype(BF16)
    evals[0].start()

    def last(s):
        y_arrival(1, s)
        dot(1, near(s))

    steps(Z, last)
    result[1] = acc[1].astype(BF16)
    evals[1].start()

    for kv in range(2):

        def drain(p):
            core_copy(kv, p).wait_send()
            y_copy(kv, p).wait_send()

            @pl.when(p != z)
            def _():
                right_copy(kv, p).wait_send()

            @pl.when((p <= z) & (z < Z - 1))
            def _():
                w_right(kv, p).wait_send()

            @pl.when((p >= z) & (z > 0))
            def _():
                w_left(kv, p).wait_send()

            w_y(kv, p, y).wait_send()
            w_core(kv, p, y, core).wait_send()
            w_core(kv, p, oy, core).wait_send()

        steps(Z, drain)
        for copy in stores(kv):
            copy.wait()
    for copy in evals:
        copy.wait()


def place(*refs):
    source, target, held = refs[:6], refs[6:12], refs[12:18]
    in_sem, out_sem = refs[18:]
    order = (2, 3, 4, 5, 0, 1)
    loads = {i: pltpu.make_async_copy(source[i], held[i], in_sem.at[i]) for i in order}
    stores = {i: pltpu.make_async_copy(held[i], target[i], out_sem.at[i]) for i in order}
    for i in order:
        loads[i].start()
    for i in order:
        loads[i].wait()
        stores[i].start()
    for i in order:
        stores[i].wait()


def body(
    tokens,
    pseudo_keys,
    pseudo_values,
    master_keys,
    moment_keys,
    master_values,
    moment_values,
    outer_hyper,
):
    replicas = lax.axis_size("replica")
    Y = 2
    Z = replicas // (2 * Y)
    width = master_keys.shape[1]
    rows = master_keys.shape[0]
    count = tokens.shape[0]
    blocks = Z * Y
    depth = 2 * rows
    if depth % 128:
        tokens = tokens.reshape(count, blocks, depth).swapaxes(0, 1)
    pseudo_keys, pseudo_values = (
        p.reshape(Z, Y, 2, rows, width) for p in (pseudo_keys, pseudo_values)
    )
    hbm = pl.BlockSpec(memory_space=pl.ANY)
    dma = pltpu.SemaphoreType.DMA
    state = jax.ShapeDtypeStruct(master_keys.shape, F32)
    evaluated = jax.ShapeDtypeStruct((count, width), BF16)
    part = pltpu.VMEM((2, Z, rows, width), BF16)
    pair = pltpu.VMEM((2, Z, Y, rows, width), BF16)
    unit = dma((2, Z))
    results = pl.pallas_call(
        functools.partial(kernel, Z, Y, replicas),
        out_shape=(evaluated, evaluated, state, state, state, state),
        in_specs=[hbm] * 7 + [pl.BlockSpec(memory_space=pltpu.SMEM)],
        out_specs=(hbm,) * 6,
        scratch_shapes=[
            pltpu.VMEM((blocks, count, depth), BF16),
            pair,
            pair,
            part,
            part,
            part,
            part,
            part,
            pltpu.VMEM((2, Z, Y, 2, rows, width), BF16),
            pltpu.VMEM((rows, width), F32),
            pltpu.VMEM((2, count, width), F32),
            pltpu.VMEM((2, count, width), BF16),
            pltpu.VMEM((2, rows, width), F32),
            pltpu.VMEM((2, rows, width), F32),
            dma((2,)),
            dma((4,)),
            dma((blocks,)),
            dma((6,)),
            unit,
            unit,
            unit,
            unit,
            unit,
            unit,
            unit,
            unit,
            unit,
            unit,
            unit,
            unit,
            dma((2, Z, Y)),
            dma((2, Z, Y)),
        ],
        compiler_params=pltpu.CompilerParams(
            collective_id=0, has_side_effects=True, vmem_limit_bytes=60 * 1024 * 1024
        ),
        name="outer_step",
    )(
        tokens,
        pseudo_keys,
        pseudo_values,
        master_keys,
        moment_keys,
        master_values,
        moment_values,
        outer_hyper,
    )
    return pl.pallas_call(
        place,
        out_shape=tuple(jax.ShapeDtypeStruct(a.shape, a.dtype) for a in results),
        in_specs=[hbm] * 6,
        out_specs=(hbm,) * 6,
        scratch_shapes=[pltpu.VMEM(a.shape, a.dtype) for a in results] + [dma((6,)), dma((6,))],
        name="place",
    )(*results)


def solution(mesh):
    rows = P(("groups", "replica"), None)
    stack = P(("groups", "replica"), None, None)
    return jax.shard_map(
        body,
        mesh=mesh,
        in_specs=(rows, stack, stack, rows, rows, rows, rows, P("groups")),
        out_specs=(rows,) * 6,
        check_vma=False,
    )
```
